32 devices in a mesh: grp: 2 (over core), row: 4 (over z), col: 4 (over y, x).
Axes of the slice: x: 2, y: 2, z: 4, core: 2. Of those that a mesh axis runs over, the one named last changes fastest.
Arguments:
- ainv_anc: bfloat16 [6144, 6144], P(('grp', 'row'), 'col'), may hold values from -12 to 12
- l_upper: bfloat16 [6144, 1024], P(('grp', 'row'), 'col'), may hold values from -0.078125 to 0.078125
- mask_upper: int32 [4, 24], replicated, may hold values from 0 to 1, as said below
- dinv_upper: float32 [256, 1024], P(None, 'col'), may hold values from -6 to 6
- l_lower: bfloat16 [6144, 1024], P(('grp', 'row'), 'col'), may hold values from -0.078125 to 0.078125
- mask_lower: int32 [4, 24], replicated, may hold values from 0 to 1, as said below
- parent: int32 [4], replicated, may hold values from 0 to 3
- lp_lower: bfloat16 [256, 1024], P(None, 'col'), may hold values from -0.375 to 0.375
- dinv_lower: float32 [256, 1024], P(None, 'col'), may hold values from -6 to 6
Outputs:
- x_upper: bfloat16 [6144, 1024], P(('grp', 'row'), 'col')
- diag_upper: bfloat16 [256, 1024], P(None, 'col')
- y_lower: bfloat16 [6144, 1024], P(('grp', 'row'), 'col')
- y_parent: bfloat16 [256, 1024], P(None, 'col')
- diag_lower: bfloat16 [256, 1024], P(None, 'col')
The draws below stay inside these ranges and needn't reach their ends.
Inputs may be any that keep to these rules, and one draw needn't show every extreme that they name: mask_upper[u, a] is 1 where ancestor block a lies in the structure of upper supernode u. mask_lower[l, a] is 1 where ancestor block a lies in the structure of lower supernode l. parent[l] is the upper supernode whose columns hold lower supernode l's parent block.
All inputs are finite; a program needn't handle non-finite values.
Results may differ from the reference program's by a relative error of at most 0.0095.
Values may be sent and summed in bfloat16 or wider, within the bound.
A program may use at most 128 MiB of HBM per device.

```python
import jax
import jax.numpy as jnp
from jax import lax

B = 256
ANC = 6144
ANCB = 24
SN = 4


def draw_ainv_anc(key, part):
    entry_key, diag_key = jax.random.split(key, 2)
    entries = jnp.clip(jax.random.normal(entry_key, (ANC, ANC), jnp.float32), -7.0, 7.0)
    diagonal = jnp.exp(jax.random.uniform(diag_key, (ANC,), jnp.float32, 0.0, 1.386))
    places = jnp.arange(ANC)
    return entries.at[places, places].add(diagonal).astype(jnp.bfloat16)


def pattern_draw(key):
    chance = jax.random.randint(key, (SN, ANCB), 0, 1000)
    threshold = 250 + 650 * jnp.arange(ANCB, dtype=jnp.int32) // max(ANCB - 1, 1)
    return (chance < threshold[None, :]).astype(jnp.int32)


def draw_mask_upper(key, part):
    return pattern_draw(jax.random.fold_in(key, 17))


def draw_mask_lower(key, part):
    return pattern_draw(jax.random.fold_in(key, 29))


def plant(drawn, own_key, smallest, high):
    dims = drawn.shape
    place = [jax.random.randint(jax.random.fold_in(own_key, axis), (), 0, dims[axis]) for axis in range(len(dims))]
    drawn = drawn.at[tuple(place)].set(smallest)
    longest = dims.index(max(dims))
    place[longest] = (place[longest] + 1) % dims[longest]
    return drawn.at[tuple(place)].set(high)


def levels(stream_key, shape, cuts, smallest, high):
    def one(position, shards_of):
        heights = jax.random.uniform(jax.random.fold_in(jax.random.fold_in(stream_key, 6), position), (shards_of,), jnp.float32, smallest / len(cuts), high / len(cuts))
        return jnp.repeat(jnp.exp(heights), shape[position] // shards_of).reshape((-1,) + (1,) * (len(shape) - position - 1))

    gain = one(*cuts[0])
    for cut in cuts[1:]:
        gain = gain * one(*cut)
    return gain


def noise(rng, extent, width, bound, cuts=(), kind=jnp.bfloat16):
    values = jax.random.normal(rng, extent, jnp.float32) * width
    if len(cuts) > 0:
        values = levels(rng, extent, cuts, -0.22, 0.18) * values
    return jnp.clip(values, min=-bound, max=bound).astype(kind)


def setup_inputs(seed: int = 0) -> dict:
    keys = jax.random.split(jax.random.key(seed), 10)
    return {
        "ainv_anc": draw_ainv_anc(jax.random.fold_in(keys[9], 71), 0),
        "l_upper": noise(keys[1], (ANC, SN * B), ANC ** -0.5, 0.078125, ((0, 8), (1, 4))),
        "mask_upper": draw_mask_upper(jax.random.fold_in(keys[9], 71), 0),
        "dinv_upper": noise(keys[3], (B, SN * B), 1.0, 6.0, ((1, 4),), jnp.float32),
        "l_lower": noise(keys[4], (ANC, SN * B), ANC ** -0.5, 0.078125, ((0, 8), (1, 4))),
        "mask_lower": draw_mask_lower(jax.random.fold_in(keys[9], 71), 0),
        "parent": plant(jax.random.randint(keys[6], (SN,), 0, SN), jax.random.fold_in(keys[6], 1), 0, SN - 1).astype(jnp.int32),
        "lp_lower": noise(keys[7], (B, SN * B), B ** -0.5, 0.375, ((1, 4),)),
        "dinv_lower": noise(keys[8], (B, SN * B), 1.0, 6.0, ((1, 4),), jnp.float32),
    }


def masked_panel(factor, pattern):
    height, breadth = factor.shape
    shaped = factor.reshape(height // B, B, breadth // B, B)
    keeping = (jnp.transpose(pattern) > 0)[:, None, :, None]
    return jnp.where(keeping, shaped, jnp.zeros((), factor.dtype)).reshape(height, breadth)


def reference(ainv_anc, l_upper, mask_upper, dinv_upper, l_lower, mask_lower, parent, lp_lower, dinv_lower):
    precise = lax.Precision.HIGHEST
    ancestor = ainv_anc.astype(jnp.float32)
    upper_masked = masked_panel(l_upper, mask_upper)
    x_upper = (-jnp.dot(ancestor, upper_masked.astype(jnp.float32), precision=precise)).astype(jnp.bfloat16)
    upper_cube = upper_masked.astype(jnp.float32).reshape(ANC, SN, B)
    x_cube = x_upper.astype(jnp.float32).reshape(ANC, SN, B)
    upper_terms = jnp.einsum("aub,auc->buc", upper_cube, x_cube, precision=precise).reshape(B, SN * B)
    diag_upper = (dinv_upper - upper_terms).astype(jnp.bfloat16)
    lower_masked = masked_panel(l_lower, mask_lower)
    lower_cube = lower_masked.astype(jnp.float32).reshape(ANC, SN, B)
    chosen = jnp.take(x_cube, parent, axis=1)
    link_cube = lp_lower.astype(jnp.float32).reshape(B, SN, B)
    coupling = jnp.einsum("alb,blc->alc", chosen, link_cube, precision=precise).reshape(ANC, SN * B)
    lower_sum = jnp.dot(ancestor, lower_masked.astype(jnp.float32), precision=precise)
    y_lower = (-(lower_sum + coupling)).astype(jnp.bfloat16)
    y_cube = y_lower.astype(jnp.float32).reshape(ANC, SN, B)
    crossed = jnp.einsum("alb,alc->blc", chosen, lower_cube, precision=precise)
    own_terms = jnp.einsum("alb,alc->blc", lower_cube, y_cube, precision=precise)
    parent_diag = jnp.take(diag_upper.astype(jnp.float32).reshape(B, SN, B), parent, axis=1)
    parent_terms = jnp.einsum("blc,cld->bld", parent_diag, link_cube, precision=precise)
    y_parent = (-(crossed + parent_terms)).astype(jnp.bfloat16)
    parent_cube = y_parent.astype(jnp.float32)
    back_terms = jnp.einsum("clb,cld->bld", link_cube, parent_cube, precision=precise)
    diag_lower = (dinv_lower.reshape(B, SN, B) - own_terms - back_terms).astype(jnp.bfloat16)
    return x_upper, diag_upper, y_lower, y_parent.reshape(B, SN * B), diag_lower.reshape(B, SN * B)
```

```python
import functools

import jax
import jax.numpy as jnp
from jax import lax
from jax.experimental import pallas as pl
from jax.experimental.pallas import tpu as pltpu
from jax.sharding import PartitionSpec as P

B = 256
MESH = pl.DeviceIdType.MESH
BF = jnp.bfloat16
F32 = jnp.float32


def tdot(a, b):
    return lax.dot_general(a, b, (((0,), (0,)), ((), ())), preferred_element_type=F32)


def land(*conds):
    out = conds[0]
    for k in conds[1:]:
        out = jnp.logical_and(out, k)
    return out


def kernel(
    G, R, C,
    a_in, lu_in, mu_ref, du_in, ll_in, ml_ref, par_ref, lp_in, dl_in,
    x_out, diagu_out, y_out, yp_out, diagl_out,
    a_ref, lu_ref, ll_ref, du_ref, dl_ref, lp_ref,
    x_ref, y_ref, ybuf, zbuf, col, acc, part, near_y, near_x, sent_y, sent_x, last_y, last_x,
    rhs, lum, llm, xrow, selbuf, chy, chosen, part3, red, dufull, dpar, ypfull, back, dlfull,
    linked, terms, in_s, out_s,
    h_ss, h_rs, t_ss, t_rs, c_rs, v_ss, r_ss, x_ss,
    ny_ss, ny_rs, nx_ss, nx_rs, ly_ss, ly_rs, lx_ss, lx_rs,
    xr_ss, xr_rs, ch_ss, ch_rs,
    red_ss, red_rs, s_ss, s_rs,
):
    g, z, c = lax.axis_index("grp"), lax.axis_index("row"), lax.axis_index("col")
    n = G * R
    q = n // C
    CX = C // G
    y, x = lax.div(c, CX), lax.rem(c, CX)
    r = g * R + z
    h = lu_ref.shape[0]
    hb = W = h // B
    S = B // n
    H2 = h // 2
    panels = (lu_ref, ll_ref)
    masks = (mu_ref, ml_ref)
    primary = y == g
    zh = lax.div(z, q)
    home = zh == x
    oy = 1 - y

    def rdev(i):
        return (lax.div(i, R), lax.rem(i, R), c)

    def pdev(yy, xx):
        return (g, z, yy * CX + xx)

    def xo(o):
        return lax.rem(x + o, CX)

    def copy(src, dst, ss, rs, dev):
        return pltpu.make_async_remote_copy(
            src_ref=src, dst_ref=dst, send_sem=ss, recv_sem=rs, device_id=dev, device_id_type=MESH
        )

    ins = [
        pltpu.make_async_copy(src, dst, in_s.at[i])
        for i, (src, dst) in enumerate(
            ((lu_in, lu_ref), (ll_in, ll_ref), (a_in, a_ref), (lp_in, lp_ref), (du_in, du_ref), (dl_in, dl_ref))
        )
    ]
    barrier = pltpu.get_barrier_semaphore()
    for o in range(1, n):
        pl.semaphore_signal(barrier, inc=1, device_id=rdev(lax.rem(r + o, n)), device_id_type=MESH)
    for o in range(1, C):
        pl.semaphore_signal(
            barrier, inc=1, device_id=(g, z, lax.rem(c + o, C)), device_id_type=MESH
        )
    for i in ins:
        i.start()
    ins[0].wait()
    ins[1].wait()
    with jax.named_scope("barrier"):
        pl.semaphore_wait(barrier, n - 1 + C - 1)

    log = []

    def cut(w):
        return pl.ds(w * B, B)

    edge = (z < R - 1, z > 0)
    away = jnp.logical_not(home)
    outer = jnp.logical_or(z == 0, z == R - 1)
    far = ((zh + 1) * q < R, zh > 0)
    zj = lax.rem(z, q)

    def side_dev(side):
        return (g, z + 1 if side == 0 else z - 1, c)

    def col_u(o, l):
        return (y if l == 0 else oy) * CX + xo(o)

    def hop_copy(p, w):
        return copy(
            panels[p].at[cut(w), :], ybuf.at[p, cut(w), :], h_ss.at[p], h_rs.at[p, w],
            (g, z, g * CX + x),
        )

    def own_src(p, l, w):
        return panels[p].at[cut(w), :] if l == 0 else ybuf.at[p, cut(w), :]

    def at_col(p, j, u, w):
        return col.at[p, j * C + u, cut(w), :]

    def along(p, j, u, side, w, src):
        return ("v", p, side), lambda: copy(
            src, at_col(p, j, u, w), v_ss.at[p, side], c_rs.at[p, j * C + u, w], side_dev(side)
        )

    def relay(p, j, u, w, src):
        return None, lambda: copy(
            src, at_col(p, j, u, w), r_ss.at[p], c_rs.at[p, j * C + u, w], (1 - g, z, c)
        )

    def cross(p, z0, l, w, src):
        u, j = col_u(0, l), lax.rem(z0, q)
        return ("x", p, 0), lambda: copy(
            src, at_col(p, j, u, w), x_ss.at[p, 0], c_rs.at[p, j * C + u, w],
            pdev(y, lax.div(z0, q)),
        )

    def through(p, z0, side, w, src):
        return ("t", p, side), lambda: copy(
            src, zbuf.at[p, z0, cut(w), :], t_ss.at[p, side], t_rs.at[p, z0, w], side_dev(side)
        )

    def own_home(p, l, w, where):
        u, src = col_u(0, l), own_src(p, l, w)
        live = {"all": home, "outer": land(home, outer), "inner": land(home, z > 0, z < R - 1)}[where]
        outs = [(edge[side], along(p, zj, u, side, w, src)) for side in range(2)]
        outs.append((None, relay(p, zj, u, w, src)))

        def local():
            k = pltpu.make_async_copy(src, at_col(p, zj, u, w), c_rs.at[p, zj * C + u, w])
            k.start()
            k.wait()

        return live, (lambda: hop_copy(p, w)) if l == 1 else None, outs, local

    def own_away(p, l, w):
        src = own_src(p, l, w)
        outs = [(None, cross(p, z, l, w, src))]
        if l == 0:
            outs += [(far[side], through(p, z, side, w, src)) for side in range(2)]
        return away, (lambda: hop_copy(p, w)) if l == 1 else None, outs, None

    def transit(p, s, side, w):
        z0 = z - s if side == 0 else z + s
        b0 = lax.div(z0, q)
        ok = z0 >= 0 if side == 0 else z0 < R
        path = (b0 + 1) * q < R if side == 0 else b0 > 0
        at = zbuf.at[p, z0, cut(w), :]
        outs = [(edge[side], through(p, z0, side, w, at)), (zh != b0, cross(p, z0, 0, w, at))]
        return land(ok, path, b0 != x), through(p, z0, side, w, at)[1], outs, None

    def arrive(p, kind, i, o, l, w):
        j = lax.rem(zj + i, q) if kind == "home" else jnp.where(z < x * q, i, q - 1 - i)
        z0 = x * q + j
        u = col_u(o, l)
        up = land(z0 <= z, edge[0])
        down = land(z0 >= z, edge[1])
        outs = []
        at = at_col(p, j, u, w)
        if o != 0 and l == 0:
            up = land(up, lax.div(z + 1, q) == x)
            down = land(down, lax.div(z - 1 + q, q) == x + 1)
        if kind == "home" or o == 0 or l == 1:
            outs = [(up, along(p, j, u, 0, w, at)), (down, along(p, j, u, 1, w, at))]
        outs.append((None, relay(p, j, u, w, at)))
        return home if kind == "home" else away, relay(p, j, u, w, at)[1], outs, None

    def emit(f, *args):
        log.append((f, args))
        live, first, outs, local = f(*args)

        def body():
            if first is not None:
                first().wait_recv()
            for cond, (_, make) in outs:
                if cond is None:
                    make().start()
                else:
                    pl.when(cond)(lambda: make().start())
            if local is not None:
                local()

        pl.when(live)(body)

    def wait_blocks(sem, p, k):
        at = col.at[p, pl.ds(0, k)]
        copy(at, at, sem, sem, rdev(r)).wait_send()

    def wait_sends():
        for p in range(2):
            wait_blocks(r_ss.at[p], p, q * C)
        count = {}
        for f, args in dict.fromkeys(log):
            if args[-1] == 0 or (f is own_home and args[-2] == 0):
                live, _, outs, _ = f(*args)
                for cond, (key, _) in outs:
                    if key is not None:
                        on = live if cond is None else land(live, cond)
                        count[key] = count.get(key, 0) + jnp.where(on, 1, 0)
        for (kind, p, side), number in sorted(count.items()):
            sem = {"v": v_ss, "x": x_ss, "t": t_ss}[kind].at[p, side]
            for k in range(1, {"v": q * C, "x": R + G, "t": R}[kind] + 1):
                pl.when(number == k)(lambda: wait_blocks(sem, p, k))

    chunks = range(W)
    others = range(1, CX)
    rest = range(1, q)
    TAU, HOP = 1.4, 3.0

    def at_home():
        ev = []

        def add(t, f, *args, slope=TAU):
            for w in chunks:
                ev.append((t + slope * w, f, (*args, w) if f is not own_home else (*args[:2], w, args[2])))

        add(0, own_home, 0, 0, "all", slope=0)
        for s in range(1, R):
            for side in range(2):
                add(HOP * s, transit, 0, s, side)
                add(4.4 + HOP * s, transit, 1, s, side)
        add(6.2, own_home, 0, 1, "all", slope=0)
        add(16.5, own_home, 1, 1, "outer", slope=0)
        add(16.7, own_home, 1, 0, "outer", slope=0)
        add(24, own_home, 1, 1, "inner", slope=0)
        add(28, own_home, 1, 0, "inner", slope=0)
        for o in others:
            add(3.1, arrive, 0, "home", 0, o, 0)
            add(8, arrive, 0, "home", 0, o, 1)
            add(19.2, arrive, 1, "home", 0, o, 0)
            add(16, arrive, 1, "home", 0, o, 1)
        for i in rest:
            add(3.05, arrive, 0, "home", i, 0, 0)
            add(11.5, arrive, 0, "home", i, 0, 1)
            add(25, arrive, 1, "home", i, 0, 1)
            add(29, arrive, 1, "home", i, 0, 0)
            for o in others:
                add(8.5, arrive, 0, "home", i, o, 0)
                add(15.7, arrive, 0, "home", i, o, 1)
                add(21, arrive, 1, "home", i, o, 1)
                add(28.5, arrive, 1, "home", i, o, 0)
        return ev

    def at_away():
        ev = []

        def add(t, f, *args, slope=TAU):
            for w in chunks:
                ev.append((t + slope * w, f, (*args, w)))

        add(0, own_away, 0, 0, slope=0)
        for s in range(1, R):
            for side in range(2):
                add(HOP * s, transit, 0, s, side)
                add(4.5 + HOP * s, transit, 1, s, side)
        add(3.2, own_away, 0, 1)
        add(6.1, own_away, 1, 0, slope=0)
        add(9, own_away, 1, 1, slope=0)
        for i in range(q):
            add(3.05 + 4.35 * i, arrive, 0, "away", i, 0, 0)
            add(11.5 + 8.4 * i, arrive, 0, "away", i, 0, 1)
            add(36.8 + 4.2 * i, arrive, 1, "away", i, 0, 1)
            add(45.2 + 4.2 * i, arrive, 1, "away", i, 0, 0)
            for o in others:
                add(9.2 + 3.1 * i, arrive, 0, "away", i, o, 0)
                add(15.7 + 8.4 * i, arrive, 0, "away", i, o, 1)
                add(23.6 + 3.9 * i, arrive, 1, "away", i, o, 0)
                add(28.3 + 4.2 * i, arrive, 1, "away", i, o, 1)
        return ev

    timed = (sorted(at_home(), key=lambda e: e[0]), sorted(at_away(), key=lambda e: e[0]))

    def events(home_to, away_to):
        for which, cond, to in ((0, home, home_to), (1, away, away_to)):
            now = [e for e in timed[which] if e[0] < to]
            timed[which][:] = timed[which][len(now):]
            if now:
                @pl.when(land(primary, cond))
                def _():
                    for _, f, args in now:
                        emit(f, *args)

    def kd(o, l):
        return l * CX + o

    def ny_copy(p, o):
        return copy(
            part.at[p, kd(o, 1), pl.ds(0, H2), :], near_y.at[p, o], ny_ss.at[p], ny_rs.at[p, o],
            pdev(oy, x),
        )

    def nx_copy(p, o, l):
        i = (CX - o) * G + l
        return copy(
            part.at[p, kd(o, l), pl.ds(H2, H2), :], near_x.at[p, i], nx_ss.at[p], nx_rs.at[p, i],
            pdev(y, xo(o)),
        )

    def ly_copy(p, o):
        return copy(
            sent_y.at[p, o], last_y.at[p, CX - o], ly_ss.at[p], ly_rs.at[p, CX - o],
            pdev(y, xo(o)),
        )

    def lx_copy(p):
        return copy(sent_x.at[p], last_x.at[p], lx_ss.at[p], lx_rs.at[p], pdev(oy, x))

    def product(p, o, l):
        u = (y if l == 0 else oy) * CX + xo(o)
        k = kd(o, l)

        @pl.when(jnp.logical_not(primary))
        def _():
            for j in range(q):
                for w in range(W):
                    relay(p, j, u, w, at_col(p, j, u, w))[1]().wait_recv()

        @pl.loop(0, q * hb)
        def _(i):
            j, t = lax.div(i, hb), lax.rem(i, hb)
            keep = masks[p][u, c * q * hb + i] > 0
            rows = pl.ds(pl.multiple_of(t * B, B), B)
            blk = col[p, j * C + u, rows, :]
            rhs[pl.ds(pl.multiple_of(i * B, B), B), :] = jnp.where(keep, blk, jnp.zeros_like(blk))

        @pl.loop(0, 2)
        def _(t):
            rows = pl.ds(pl.multiple_of(t * H2, H2), H2)
            v = jnp.dot(a_ref[rows, :], rhs[...], preferred_element_type=F32)
            acc[p, k, rows, :] = v
            part[p, k, rows, :] = v.astype(BF)

        if l == 1:
            ny_copy(p, o).start()
        if o != 0:
            nx_copy(p, o, l).start()

    top, low = pl.ds(0, H2), pl.ds(H2, H2)

    def second(p):
        for o in range(1, CX):
            ny_copy(p, o).wait_recv()
            sent_y[p, o] = (acc[p, kd(o, 0), top, :] + near_y[p, o].astype(F32)).astype(BF)
            ly_copy(p, o).start()
        v = acc[p, kd(0, 1), low, :]
        for o in range(1, CX):
            nx_copy(p, CX - o, 1).wait_recv()
            v = v + near_x[p, o * G + 1].astype(F32)
        sent_x[p] = v.astype(BF)
        lx_copy(p).start()

    def total(p):
        ny_copy(p, 0).wait_recv()
        v = acc[p, 0, top, :] + near_y[p, 0].astype(F32)
        for o in range(1, CX):
            ly_copy(p, CX - o).wait_recv()
            v = v + last_y[p, o].astype(F32)
        w = acc[p, 0, low, :]
        for o in range(1, CX):
            nx_copy(p, CX - o, 0).wait_recv()
            w = w + near_x[p, o * G].astype(F32)
        lx_copy(p).wait_recv()
        w = w + last_x[p].astype(F32)
        return (-v).astype(BF), (-w).astype(BF)

    def red_copy(k, o):
        i = lax.rem(r + o, n)
        return copy(
            part3.at[k, pl.ds(pl.multiple_of(i * S, S), S), :], red.at[k, r],
            red_ss.at[k], red_rs.at[k], rdev(i),
        )

    def send_sum(k):
        red[k, r] = part3[k, pl.ds(pl.multiple_of(r * S, S), S), :]
        for o in range(1, n):
            red_copy(k, o).start()

    def all_red(k):
        at = red.at[k, pl.ds(0, n - 1)]
        return copy(at, at, red_ss.at[k], red_rs.at[k], rdev(r))

    def take_sum(k):
        all_red(k).wait_recv()
        v = red[k, 0].astype(F32)
        for i in range(1, n):
            v = v + red[k, i].astype(F32)
        return v

    mine = pl.ds(pl.multiple_of(r * S, S), S)

    def spread(i, buf):
        for o in range(1, n):
            copy(
                buf.at[mine, :], buf.at[mine, :], s_ss.at[i], s_rs.at[i], rdev(lax.rem(r + o, n))
            ).start()

    def all_spread(i, buf):
        at = buf.at[pl.ds(0, (n - 1) * S), :]
        return copy(at, at, s_ss.at[i], s_rs.at[i], rdev(r))

    def dp_copy(o):
        return copy(
            dpar.at[c], dpar.at[c], s_ss.at[3], s_rs.at[3], (g, z, lax.rem(c + o, C))
        )

    def all_dp():
        at = dpar.at[pl.ds(0, C - 1)]
        return copy(at, at, s_ss.at[3], s_rs.at[3], rdev(r))

    def xr_copy(o, w):
        return copy(
            x_ref.at[cut(w), :], xrow.at[CX - o, cut(w), :], xr_ss.at[0],
            xr_rs.at[CX - o, w], pdev(y, xo(o)),
        )

    def ch_copy(w):
        return copy(selbuf.at[cut(w), :], chy.at[cut(w), :], ch_ss.at[0], ch_rs.at[w], pdev(oy, x))

    def pick(who, base, w):
        v = base
        for o in range(CX):
            src = x_ref if o == 0 else xrow.at[o]
            v = jnp.where(who == y * CX + xo(o), src[cut(w), :], v)
        return v

    def out_copy(i, src, dst):
        return pltpu.make_async_copy(src, dst, out_s.at[i])

    def step(name, f, cond=None):
        with jax.named_scope(name):
            if cond is None:
                f()
            else:
                pl.when(cond)(f)

    def start_hops():
        for p in range(2):
            for w in range(W):
                hop_copy(p, w).start()

    def mask_own():
        @pl.loop(0, hb)
        def _(t):
            rows = pl.ds(pl.multiple_of(t * B, B), B)
            ub, lb = lu_ref[rows, :], ll_ref[rows, :]
            lum[rows, :] = jnp.where(mu_ref[c, r * hb + t] > 0, ub, jnp.zeros_like(ub))
            llm[rows, :] = jnp.where(ml_ref[c, r * hb + t] > 0, lb, jnp.zeros_like(lb))

    def x_final():
        xt, xl = total(0)
        x_ref[top, :] = xt
        x_ref[low, :] = xl
        for w in range(W):
            for o in range(1, CX):
                xr_copy(o, w).start()
        out_copy(0, x_ref, x_out).start()
        part3[0] = tdot(lum[...], x_ref[...]).astype(BF)
        send_sum(0)

    def choose_send():
        to = par_ref[oy * CX + x]
        for w in range(W):
            for o in range(1, CX):
                xr_copy(CX - o, w).wait_recv()
            selbuf[cut(w), :] = pick(to, x_ref[cut(w), :], w)
            ch_copy(w).start()

    def diag_upper():
        dslice = (du_ref[mine, :] - take_sum(0)).astype(BF)
        dufull[mine, :] = dslice
        dpar[c] = dslice
        for o in range(1, C):
            dp_copy(o).start()
        spread(0, dufull)

    here = par_ref[c]

    def choose_take():
        for w in range(W):
            ch_copy(w).wait_recv()
            chosen[cut(w), :] = pick(here, chy[cut(w), :], w)

    def crossed():
        part3[1] = tdot(chosen[...], llm[...]).astype(BF)
        send_sum(1)

    def coupling():
        @pl.loop(0, hb)
        def _(t):
            rows = pl.ds(pl.multiple_of(t * B, B), B)
            v = jnp.dot(chosen[rows, :], lp_ref[...], preferred_element_type=F32)
            acc[1, 0, rows, :] += v
            linked[rows, :] = v.astype(BF)

    def parent_terms():
        all_dp().wait_recv()
        v = jnp.dot(dpar[here], lp_ref[...], preferred_element_type=F32)
        terms[...] = v
        back[...] = -tdot(linked[...], llm[...]) - tdot(lp_ref[mine, :], v.astype(BF))

    def y_final():
        yt, yl = total(1)
        y_ref[top, :] = yt
        y_ref[low, :] = yl
        part3[2] = (tdot(llm[...], y_ref[...]) + back[...]).astype(BF)
        send_sum(2)
        out_copy(1, y_ref, y_out).start()

    def y_parent():
        ypfull[mine, :] = (-(take_sum(1) + terms[...])).astype(BF)
        spread(1, ypfull)

    def diag_lower():
        dlfull[mine, :] = (dl_ref[mine, :] - take_sum(2)).astype(BF)
        spread(2, dlfull)

    def gather_upper():
        all_spread(0, dufull).wait_recv()
        out_copy(2, dufull, diagu_out).start()

    def gather_parent():
        all_spread(1, ypfull).wait_recv()
        out_copy(3, ypfull, yp_out).start()

    def gather_lower():
        all_spread(2, dlfull).wait_recv()
        out_copy(4, dlfull, diagl_out).start()

    def wait_ins():
        for i in ins[2:]:
            i.wait()

    def products(p, l):
        for o in range(1, CX):
            product(p, o, l)

    pl.when(jnp.logical_not(primary))(start_hops)
    step("ev0", lambda: events(0.1, 0.1))
    step("mask", mask_own)
    step("ev1", lambda: events(11.9, 10.9))
    wait_ins()
    step("prod_u1", lambda: product(0, 0, 0))
    step("ev2", lambda: events(13.5, 16.0))
    step("prod_u4", lambda: products(0, 0))
    step("ev3", lambda: events(15.6, 23.5))
    step("prod_u2", lambda: product(0, 0, 1))
    step("ev4", lambda: events(20.2, 27.2))
    step("prod_u3", lambda: products(0, 1))
    step("ev5", lambda: events(99, 36.5))
    step("lprod_u3", lambda: products(1, 1))
    step("lprod_u4", lambda: products(1, 0))
    step("second", lambda: second(0))
    step("ev6", lambda: events(99, 44.5))
    step("lprod_u2", lambda: product(1, 0, 1))
    step("x_final", x_final)
    step("second_l", lambda: second(1))
    step("ev7", lambda: events(99, 48.5))
    step("choose_send", choose_send)
    step("diag_upper", diag_upper)
    step("ev8", lambda: events(99, 99))
    step("lprod_u1", lambda: product(1, 0, 0))
    step("choose_take", choose_take)
    step("crossed", crossed)
    step("coupling", coupling)
    step("parent_terms", parent_terms)
    step("y_final", y_final)
    step("y_parent", y_parent)
    step("diag_lower", diag_lower)
    step("gather_upper", gather_upper)
    step("gather_parent", gather_parent)
    step("gather_lower", gather_lower)

    def finish():
        @pl.when(primary)
        def _():
            wait_sends()

        @pl.when(jnp.logical_not(primary))
        def _():
            for p in range(2):
                copy(ybuf.at[p], ybuf.at[p], h_ss.at[p], h_ss.at[p], rdev(r)).wait_send()

        def sent(sem, at):
            copy(at, at, sem, sem, rdev(r)).wait_send()

        for p in range(2):
            sent(ny_ss.at[p], near_y.at[p])
            sent(nx_ss.at[p], near_x.at[p, pl.ds(0, (CX - 1) * G)])
            sent(ly_ss.at[p], last_y.at[p, pl.ds(0, CX - 1)])
            sent(lx_ss.at[p], last_x.at[p])
        sent(xr_ss.at[0], xrow.at[pl.ds(0, CX - 1)])
        sent(ch_ss.at[0], chy)
        for k in range(3):
            all_red(k).wait_send()
        for i, buf in enumerate((dufull, ypfull, dlfull)):
            all_spread(i, buf).wait_send()
        all_dp().wait_send()
        for i, (src, dst) in enumerate(
            ((x_ref, x_out), (y_ref, y_out), (dufull, diagu_out), (ypfull, yp_out), (dlfull, diagl_out))
        ):
            out_copy(i, src, dst).wait()

    step("finish", finish)


def on_device(G, R, C, a, lu, mu, du, ll, ml, par, lp, dl):
    h = lu.shape[0]
    n = G * R
    q = n // C
    S = B // n
    CX = C // G
    W = h // B
    H2 = h // 2
    hbm = pl.BlockSpec(memory_space=pl.ANY)
    sm = pl.BlockSpec(memory_space=pltpu.SMEM)
    dma = pltpu.SemaphoreType.DMA
    small = jax.ShapeDtypeStruct((B, B), BF)
    tall = jax.ShapeDtypeStruct((h, B), BF)
    vm = pltpu.VMEM
    return pl.pallas_call(
        functools.partial(kernel, G, R, C),
        out_shape=(tall, small, tall, small, small),
        in_specs=[hbm, hbm, sm, hbm, hbm, sm, sm, hbm, hbm],
        out_specs=(hbm,) * 5,
        scratch_shapes=[
            vm(a.shape, BF), vm((h, B), BF), vm((h, B), BF), vm((B, B), F32), vm((B, B), F32), vm((B, B), BF),
            vm((h, B), BF), vm((h, B), BF),
            vm((2, h, B), BF),
            vm((2, R, h, B), BF),
            vm((2, q * C, h, B), BF),
            vm((2, C, h, B), F32),
            vm((2, C, h, B), BF),
            vm((2, CX, H2, B), BF),
            vm((2, CX * G, H2, B), BF),
            vm((2, CX, H2, B), BF),
            vm((2, H2, B), BF),
            vm((2, CX, H2, B), BF),
            vm((2, H2, B), BF),
            vm((q * h, B), BF),
            vm((h, B), BF), vm((h, B), BF),
            vm((CX, h, B), BF), vm((h, B), BF), vm((h, B), BF), vm((h, B), BF),
            vm((3, B, B), BF),
            vm((3, n, S, B), BF),
            vm((B, B), BF),
            vm((C, S, B), BF),
            vm((B, B), BF),
            vm((B, B), F32),
            vm((B, B), BF),
            vm((h, B), BF), vm((S, B), F32),
            dma((6,)), dma((5,)),
            dma((2,)), dma((2, W)), dma((2, 2)), dma((2, R, W)),
            dma((2, q * C, W)), dma((2, 2)), dma((2,)), dma((2, 1)),
            dma((2,)), dma((2, CX)), dma((2,)), dma((2, CX * G)),
            dma((2,)), dma((2, CX)), dma((2,)), dma((2,)),
            dma((1,)), dma((CX, W)), dma((1,)), dma((W,)),
            dma((3,)), dma((3,)), dma((4,)), dma((4,)),
        ],
        compiler_params=pltpu.CompilerParams(
            collective_id=0, has_side_effects=True, vmem_limit_bytes=60 * 1024 * 1024
        ),
    )(a, lu, mu, du, ll, ml, par, lp, dl)


def solution(mesh):
    tall, wide = P(("grp", "row"), "col"), P(None, "col")
    return jax.shard_map(
        functools.partial(
            on_device, mesh.shape["grp"], mesh.shape["row"], mesh.shape["col"]
        ),
        mesh=mesh,
        in_specs=(tall, tall, P(), wide, tall, P(), P(), wide, wide),
        out_specs=(tall, wide, tall, wide, wide),
        check_vma=False,
    )
```

```python
import functools

import jax
import jax.numpy as jnp
from jax import lax
from jax.experimental import pallas as pl
from jax.experimental.pallas import tpu as pltpu
from jax.sharding import PartitionSpec as P

B = 256
MESH = pl.DeviceIdType.MESH
BF = jnp.bfloat16
F32 = jnp.float32


def tdot(a, b):
    return lax.dot_general(a, b, (((0,), (0,)), ((), ())), preferred_element_type=F32)


def land(*conds):
    out = conds[0]
    for k in conds[1:]:
        out = jnp.logical_and(out, k)
    return out


TAU = 1.4


def plan(kind, R, q, CX, W):
    ev = []

    def add(t, name, *args, slope=TAU):
        for w in range(W):
            ev.append((t + slope * w, name, args, w))

    def at(t, name, *args):
        add(t, name, *args, slope=0.001)

    others = range(1, CX)
    inner = kind[1] == "I"
    if CX != 2:
        for p, l in ((0, 0), (0, 1), (1, 0), (1, 1)):
            if kind[0] == "H":
                for part in ("far", "near"):
                    at(0, "own", p, l, part)
            else:
                at(0, "away", p, l)
        for p in range(2):
            for s in range(1, R):
                for side in range(2):
                    at(1 + p + s / R, "transit", p, s, side)
            t = (5, 33)[p]
            if kind[0] == "H":
                for part in ("far", "near"):
                    for o in others:
                        for l in range(2):
                            at(t, "arrive", p, "home", 0, o, l, part)
            for l in range(2):
                for o in range(CX):
                    for i in range(0 if kind[0] == "A" else 1, q):
                        at(t + 1 + l + 0.1 * o, "arrive", p, ("away" if kind[0] == "A" else "home"), i, o, l, "far")
        return sorted(ev, key=lambda e: e[0])
    if kind[0] == "H":
        at(0, "own", 0, 0, "far")
        for s in range(1, R):
            for side in range(2):
                add((0 if inner else 0.1) + 3.9 * s, "transit", 0, s, side)
                add(9.1 + 4 * s if inner else 25.2 + 4.1 * s, "transit", 1, s, side)
        if inner:
            at(7, "own", 0, 1, "far")
            at(12.2, "own", 0, 0, "near")
            at(12.6, "own", 0, 1, "near")
            at(24.8, "own", 1, 1, "far")
            at(28.7, "own", 1, 0, "far")
            at(28.8, "own", 1, 1, "near")
            at(28.9, "own", 1, 0, "near")
        else:
            at(0.1, "own", 0, 0, "near")
            add(4.0, "own", 0, 1, "far")
            add(4.01, "own", 0, 1, "near")
            at(18.2, "own", 1, 1, "far")
            at(18.3, "own", 1, 1, "near")
            at(18.4, "own", 1, 0, "far")
            at(18.5, "own", 1, 0, "near")
        for o in others:
            add(4.05, "arrive", 0, "home", 0, o, 0, "far")
            add(8.0, "arrive", 0, "home", 0, o, 1, "far")
            if inner:
                at(12.4, "arrive", 0, "home", 0, o, 0, "near")
                at(12.8, "arrive", 0, "home", 0, o, 1, "near")
                at(17, "arrive", 1, "home", 0, o, 1, "far")
                at(19.9, "arrive", 1, "home", 0, o, 0, "far")
                at(25, "arrive", 1, "home", 0, o, 1, "near")
                at(25.1, "arrive", 1, "home", 0, o, 0, "near")
            else:
                add(8.01, "arrive", 0, "home", 0, o, 1, "near")
                at(11.5, "arrive", 0, "home", 0, o, 0, "near")
                add(15.2, "arrive", 1, "home", 0, o, 1, "far")
                add(15.21, "arrive", 1, "home", 0, o, 1, "near")
                at(20.2, "arrive", 1, "home", 0, o, 0, "far")
                at(20.3, "arrive", 1, "home", 0, o, 0, "near")
        for i in range(1, q):
            first = (4.02, 9.0, 12.5, 16.5) if inner else (16.5, 25.0, 29.2, 20.8)
            last = (29.2, 25.0, 20.7, 33.5) if inner else (54.3, 50.1, 41.6, 45.8)
            for p, (t1, t2, t3, t4) in ((0, first), (1, last)):
                add(t1, "arrive", p, "home", i, 0, 0, "far")
                add(t2, "arrive", p, "home", i, 0, 1, "far")
                for o in others:
                    add(t3, "arrive", p, "home", i, o, 1, "far")
                    add(t4, "arrive", p, "home", i, o, 0, "far")
    else:
        at(0, "away", 0, 0)
        for s in range(1, R):
            for side in range(2):
                add(0.1 + 3.9 * s, "transit", 0, s, side)
                add(11.5 + 3.9 * s, "transit", 1, s, side)
        add(4.1, "away", 0, 1)
        add(8.5, "away", 1, 1)
        at(11.6, "away", 1, 0)
        d = 0 if inner else 3.9
        for i in range(q):
            add(4.05 + d + 3.95 * i, "arrive", 0, "away", i, 0, 0, "far")
            add(12.1 + d + 8.5 * i, "arrive", 0, "away", i, 0, 1, "far")
            add(37.5 + d + 4.2 * i, "arrive", 1, "away", i, 0, 1, "far")
            add(46 + d + 4.2 * i, "arrive", 1, "away", i, 0, 0, "far")
            for o in others:
                add(8.2 + d + 4 * i, "arrive", 0, "away", i, o, 0, "far")
                add(16.4 + d + 8.4 * i, "arrive", 0, "away", i, o, 1, "far")
                if inner:
                    at(27.9 + 0.1 * i, "arrive", 1, "away", i, o, 0, "far")
                else:
                    add(37.2 + 4.2 * i, "arrive", 1, "away", i, o, 0, "far")
                add(29 + d + 4.2 * i, "arrive", 1, "away", i, o, 1, "far")
    return sorted(ev, key=lambda e: e[0])


def kernel(
    G, R, C,
    a_in, lu_in, mu_ref, du_in, ll_in, ml_ref, par_ref, lp_in, dl_in,
    x_out, diagu_out, y_out, yp_out, diagl_out,
    a_ref, lu_ref, ll_ref, du_ref, dl_ref, lp_ref,
    x_ref, y_ref, ybuf, zbuf, col, acc, part, near_y, near_x, sent_y, sent_x, last_y, last_x,
    rhs, lum, llm, xrow, selbuf, chy, chosen, part3, red, dufull, dpar, ypfull, back, dlfull,
    linked, terms, in_s, out_s,
    h_ss, h_rs, t_ss, t_rs, c_rs, v_ss, r_ss, x_ss,
    ny_ss, ny_rs, nx_ss, nx_rs, ly_ss, ly_rs, lx_ss, lx_rs,
    xr_ss, xr_rs, ch_ss, ch_rs,
    red_ss, red_rs, s_ss, s_rs,
):
    g, z, c = lax.axis_index("grp"), lax.axis_index("row"), lax.axis_index("col")
    n = G * R
    q = n // C
    CX = C // G
    y, x = lax.div(c, CX), lax.rem(c, CX)
    r = g * R + z
    h = lu_ref.shape[0]
    hb = W = h // B
    S = B // n
    H2 = h // 2
    panels = (lu_ref, ll_ref)
    masks = (mu_ref, ml_ref)
    primary = y == g
    zh = lax.div(z, q)
    home = zh == x
    oy = 1 - y

    def rdev(i):
        return (lax.div(i, R), lax.rem(i, R), c)

    def pdev(yy, xx):
        return (g, z, yy * CX + xx)

    def xo(o):
        return lax.rem(x + o, CX)

    def copy(src, dst, ss, rs, dev):
        return pltpu.make_async_remote_copy(
            src_ref=src, dst_ref=dst, send_sem=ss, recv_sem=rs, device_id=dev, device_id_type=MESH
        )

    ins = [
        pltpu.make_async_copy(src, dst, in_s.at[i])
        for i, (src, dst) in enumerate(
            ((lu_in, lu_ref), (ll_in, ll_ref), (a_in, a_ref), (lp_in, lp_ref), (du_in, du_ref), (dl_in, dl_ref))
        )
    ]
    barrier = pltpu.get_barrier_semaphore()
    for o in range(1, n):
        pl.semaphore_signal(barrier, inc=1, device_id=rdev(lax.rem(r + o, n)), device_id_type=MESH)
    for o in range(1, C):
        pl.semaphore_signal(
            barrier, inc=1, device_id=(g, z, lax.rem(c + o, C)), device_id_type=MESH
        )
    for i in ins:
        i.start()
    ins[0].wait()
    ins[1].wait()
    with jax.named_scope("barrier"):
        pl.semaphore_wait(barrier, n - 1 + C - 1)

    log = []

    def cut(w):
        return pl.ds(w * B, B)

    edge = (z < R - 1, z > 0)
    away = jnp.logical_not(home)
    outer = jnp.logical_or(z == 0, z == R - 1)
    far = ((zh + 1) * q < R, zh > 0)
    zj = lax.rem(z, q)

    def side_dev(side):
        return (g, z + 1 if side == 0 else z - 1, c)

    def col_u(o, l):
        return (y if l == 0 else oy) * CX + xo(o)

    def hop_copy(p, w):
        return copy(
            panels[p].at[cut(w), :], ybuf.at[p, cut(w), :], h_ss.at[p], h_rs.at[p, w],
            (g, z, g * CX + x),
        )

    def own_src(p, l, w):
        return panels[p].at[cut(w), :] if l == 0 else ybuf.at[p, cut(w), :]

    def at_col(p, j, u, w):
        return col.at[p, j * C + u, cut(w), :]

    def along(p, j, u, side, w, src):
        return ("v", p, side), lambda: copy(
            src, at_col(p, j, u, w), v_ss.at[p, side], c_rs.at[p, j * C + u, w], side_dev(side)
        )

    def relay(p, j, u, w, src):
        return None, lambda: copy(
            src, at_col(p, j, u, w), r_ss.at[p], c_rs.at[p, j * C + u, w], (1 - g, z, c)
        )

    def cross(p, z0, l, w, src):
        u, j = col_u(0, l), lax.rem(z0, q)
        return ("x", p, 0), lambda: copy(
            src, at_col(p, j, u, w), x_ss.at[p, 0], c_rs.at[p, j * C + u, w],
            pdev(y, lax.div(z0, q)),
        )

    def through(p, z0, side, w, src):
        return ("t", p, side), lambda: copy(
            src, zbuf.at[p, z0, cut(w), :], t_ss.at[p, side], t_rs.at[p, z0, w], side_dev(side)
        )

    near_side = (lax.div(z + 1, q) == x, lax.div(z - 1 + q, q) == x + 1)

    def own(p, l, part, w):
        u, src = col_u(0, l), own_src(p, l, w)

        def sides(near):
            return [
                (
                    land(edge[k], near_side[k] if near else jnp.logical_not(near_side[k])),
                    along(p, zj, u, k, w, src),
                )
                for k in range(2)
            ]

        if part == "near":
            return home, None, sides(True), None

        def local():
            k = pltpu.make_async_copy(src, at_col(p, zj, u, w), c_rs.at[p, zj * C + u, w])
            k.start()
            k.wait()

        outs = sides(False) + [(None, relay(p, zj, u, w, src))]
        return home, (lambda: hop_copy(p, w)) if l == 1 else None, outs, local

    def away_own(p, l, w):
        src = own_src(p, l, w)
        outs = [(None, cross(p, z, l, w, src))]
        if l == 0:
            outs += [(far[side], through(p, z, side, w, src)) for side in range(2)]
        return away, (lambda: hop_copy(p, w)) if l == 1 else None, outs, None

    def transit(p, s, side, w):
        z0 = z - s if side == 0 else z + s
        b0 = lax.div(z0, q)
        ok = z0 >= 0 if side == 0 else z0 < R
        path = (b0 + 1) * q < R if side == 0 else b0 > 0
        at = zbuf.at[p, z0, cut(w), :]
        outs = [(edge[side], through(p, z0, side, w, at)), (zh != b0, cross(p, z0, 0, w, at))]
        return land(ok, path, b0 != x), through(p, z0, side, w, at)[1], outs, None

    def arrive(p, kind, i, o, l, part, w):
        j = lax.rem(zj + i, q) if kind == "home" else jnp.where(z < x * q, i, q - 1 - i)
        z0 = x * q + j
        u = col_u(o, l)
        at = at_col(p, j, u, w)
        side = (land(z0 <= z, edge[0]), land(z0 >= z, edge[1]))
        late = o != 0 and l == 0
        outs = []
        for k in range(2):
            step_to = along(p, j, u, k, w, at)
            if kind == "away":
                if not late:
                    outs.append((side[k], step_to))
            elif i == 0:
                if part == "near":
                    outs.append((land(side[k], near_side[k]), step_to))
                elif not late:
                    outs.append((land(side[k], jnp.logical_not(near_side[k])), step_to))
            else:
                outs.append((land(side[k], near_side[k]) if late else side[k], step_to))
        live = home if kind == "home" else away
        if part == "near":
            return live, None, outs, None
        outs.append((None, relay(p, j, u, w, at)))
        return live, relay(p, j, u, w, at)[1], outs, None

    def emit(f, *args):
        log.append((f, args))
        live, first, outs, local = f(*args)

        def body():
            if first is not None:
                first().wait_recv()
            for cond, (_, make) in outs:
                if cond is None:
                    make().start()
                else:
                    pl.when(cond)(lambda: make().start())
            if local is not None:
                local()

        pl.when(live)(body)

    def wait_blocks(sem, p, k):
        at = col.at[p, pl.ds(0, k)]
        copy(at, at, sem, sem, rdev(r)).wait_send()

    def wait_sends():
        for p in range(2):
            wait_blocks(r_ss.at[p], p, q * C)
        count = {}
        for f, args in dict.fromkeys(log):
            if args[-1] == 0:
                live, _, outs, _ = f(*args)
                for cond, (key, _) in outs:
                    if key is not None:
                        on = live if cond is None else land(live, cond)
                        count[key] = count.get(key, 0) + jnp.where(on, 1, 0)
        for (kind, p, side), number in sorted(count.items()):
            sem = {"v": v_ss, "x": x_ss, "t": t_ss}[kind].at[p, side]
            for k in range(1, {"v": q * C, "x": R + G, "t": R}[kind] + 1):
                pl.when(number == k)(lambda: wait_blocks(sem, p, k))

    handlers = {"own": own, "away": away_own, "transit": transit, "arrive": arrive}
    kinds = ("HI", "HO", "AI", "AO")
    timed = {k: plan(k, R, q, CX, W) for k in kinds}
    is_kind = {
        "HI": land(home, jnp.logical_not(outer)), "HO": land(home, outer),
        "AI": land(away, jnp.logical_not(outer)), "AO": land(away, outer),
    }

    def events(*until):
        for k, to in zip(kinds, until):
            now = [e for e in timed[k] if e[0] < to]
            timed[k] = timed[k][len(now):]
            if now:
                @pl.when(land(primary, is_kind[k]))
                def _():
                    for _, name, args, w in now:
                        emit(handlers[name], *args, w)

    def kd(o, l):
        return l * CX + o

    def ny_copy(p, o):
        return copy(
            part.at[p, kd(o, 1), pl.ds(0, H2), :], near_y.at[p, o], ny_ss.at[p], ny_rs.at[p, o],
            pdev(oy, x),
        )

    def nx_copy(p, o, l):
        i = (CX - o) * G + l
        return copy(
            part.at[p, kd(o, l), pl.ds(H2, H2), :], near_x.at[p, i], nx_ss.at[p], nx_rs.at[p, i],
            pdev(y, xo(o)),
        )

    def ly_copy(p, o):
        return copy(
            sent_y.at[p, o], last_y.at[p, CX - o], ly_ss.at[p], ly_rs.at[p, CX - o],
            pdev(y, xo(o)),
        )

    def lx_copy(p):
        return copy(sent_x.at[p], last_x.at[p], lx_ss.at[p], lx_rs.at[p], pdev(oy, x))

    def product(p, o, l):
        u = (y if l == 0 else oy) * CX + xo(o)
        k = kd(o, l)

        @pl.when(jnp.logical_not(primary))
        def _():
            for j in range(q):
                for w in range(W):
                    relay(p, j, u, w, at_col(p, j, u, w))[1]().wait_recv()

        @pl.loop(0, q * hb)
        def _(i):
            j, t = lax.div(i, hb), lax.rem(i, hb)
            keep = masks[p][u, c * q * hb + i] > 0
            rows = pl.ds(pl.multiple_of(t * B, B), B)
            blk = col[p, j * C + u, rows, :]
            rhs[pl.ds(pl.multiple_of(i * B, B), B), :] = jnp.where(keep, blk, jnp.zeros_like(blk))

        @pl.loop(0, 2)
        def _(t):
            rows = pl.ds(pl.multiple_of(t * H2, H2), H2)
            v = jnp.dot(a_ref[rows, :], rhs[...], preferred_element_type=F32)
            acc[p, k, rows, :] = v
            part[p, k, rows, :] = v.astype(BF)

        if l == 1:
            ny_copy(p, o).start()
        if o != 0:
            nx_copy(p, o, l).start()

    top, low = pl.ds(0, H2), pl.ds(H2, H2)

    def second(p):
        for o in range(1, CX):
            ny_copy(p, o).wait_recv()
            sent_y[p, o] = (acc[p, kd(o, 0), top, :] + near_y[p, o].astype(F32)).astype(BF)
            ly_copy(p, o).start()
        v = acc[p, kd(0, 1), low, :]
        for o in range(1, CX):
            nx_copy(p, CX - o, 1).wait_recv()
            v = v + near_x[p, o * G + 1].astype(F32)
        sent_x[p] = v.astype(BF)
        lx_copy(p).start()

    def total(p):
        ny_copy(p, 0).wait_recv()
        v = acc[p, 0, top, :] + near_y[p, 0].astype(F32)
        for o in range(1, CX):
            ly_copy(p, CX - o).wait_recv()
            v = v + last_y[p, o].astype(F32)
        w = acc[p, 0, low, :]
        for o in range(1, CX):
            nx_copy(p, CX - o, 0).wait_recv()
            w = w + near_x[p, o * G].astype(F32)
        lx_copy(p).wait_recv()
        w = w + last_x[p].astype(F32)
        return (-v).astype(BF), (-w).astype(BF)

    def red_copy(k, o):
        i = lax.rem(r + o, n)
        return copy(
            part3.at[k, pl.ds(pl.multiple_of(i * S, S), S), :], red.at[k, r],
            red_ss.at[k], red_rs.at[k], rdev(i),
        )

    def send_sum(k):
        red[k, r] = part3[k, pl.ds(pl.multiple_of(r * S, S), S), :]
        for o in range(1, n):
            red_copy(k, o).start()

    def all_red(k):
        at = red.at[k, pl.ds(0, n - 1)]
        return copy(at, at, red_ss.at[k], red_rs.at[k], rdev(r))

    def take_sum(k):
        all_red(k).wait_recv()
        v = red[k, 0].astype(F32)
        for i in range(1, n):
            v = v + red[k, i].astype(F32)
        return v

    mine = pl.ds(pl.multiple_of(r * S, S), S)

    def spread(i, buf):
        for o in range(1, n):
            copy(
                buf.at[mine, :], buf.at[mine, :], s_ss.at[i], s_rs.at[i], rdev(lax.rem(r + o, n))
            ).start()

    def all_spread(i, buf):
        at = buf.at[pl.ds(0, (n - 1) * S), :]
        return copy(at, at, s_ss.at[i], s_rs.at[i], rdev(r))

    def dp_copy(o):
        return copy(
            dpar.at[c], dpar.at[c], s_ss.at[3], s_rs.at[3], (g, z, lax.rem(c + o, C))
        )

    def all_dp():
        at = dpar.at[pl.ds(0, C - 1)]
        return copy(at, at, s_ss.at[3], s_rs.at[3], rdev(r))

    def xr_copy(o, w):
        return copy(
            x_ref.at[cut(w), :], xrow.at[CX - o, cut(w), :], xr_ss.at[0],
            xr_rs.at[CX - o, w], pdev(y, xo(o)),
        )

    def ch_copy(w):
        return copy(selbuf.at[cut(w), :], chy.at[cut(w), :], ch_ss.at[0], ch_rs.at[w], pdev(oy, x))

    def pick(who, base, w):
        v = base
        for o in range(CX):
            src = x_ref if o == 0 else xrow.at[o]
            v = jnp.where(who == y * CX + xo(o), src[cut(w), :], v)
        return v

    def out_copy(i, src, dst):
        return pltpu.make_async_copy(src, dst, out_s.at[i])

    def step(name, f, cond=None):
        with jax.named_scope(name):
            if cond is None:
                f()
            else:
                pl.when(cond)(f)

    def start_hops():
        for p in range(2):
            for w in range(W):
                hop_copy(p, w).start()

    def mask_own():
        @pl.loop(0, hb)
        def _(t):
            rows = pl.ds(pl.multiple_of(t * B, B), B)
            ub, lb = lu_ref[rows, :], ll_ref[rows, :]
            lum[rows, :] = jnp.where(mu_ref[c, r * hb + t] > 0, ub, jnp.zeros_like(ub))
            llm[rows, :] = jnp.where(ml_ref[c, r * hb + t] > 0, lb, jnp.zeros_like(lb))

    def x_final():
        xt, xl = total(0)
        x_ref[top, :] = xt
        x_ref[low, :] = xl
        for w in range(W):
            for o in range(1, CX):
                xr_copy(o, w).start()
        out_copy(0, x_ref, x_out).start()
        part3[0] = tdot(lum[...], x_ref[...]).astype(BF)
        send_sum(0)

    def choose_send():
        to = par_ref[oy * CX + x]
        for w in range(W):
            for o in range(1, CX):
                xr_copy(CX - o, w).wait_recv()
            selbuf[cut(w), :] = pick(to, x_ref[cut(w), :], w)
            ch_copy(w).start()

    def diag_upper():
        dslice = (du_ref[mine, :] - take_sum(0)).astype(BF)
        dufull[mine, :] = dslice
        dpar[c] = dslice
        for o in range(1, C):
            dp_copy(o).start()
        spread(0, dufull)

    here = par_ref[c]

    def choose_take():
        for w in range(W):
            ch_copy(w).wait_recv()
            chosen[cut(w), :] = pick(here, chy[cut(w), :], w)

    def crossed():
        part3[1] = tdot(chosen[...], llm[...]).astype(BF)
        send_sum(1)

    def coupling():
        @pl.loop(0, hb)
        def _(t):
            rows = pl.ds(pl.multiple_of(t * B, B), B)
            v = jnp.dot(chosen[rows, :], lp_ref[...], preferred_element_type=F32)
            acc[1, 0, rows, :] += v
            linked[rows, :] = v.astype(BF)

    def parent_terms():
        all_dp().wait_recv()
        v = jnp.dot(dpar[here], lp_ref[...], preferred_element_type=F32)
        terms[...] = v
        back[...] = -tdot(linked[...], llm[...]) - tdot(lp_ref[mine, :], v.astype(BF))

    def y_final():
        yt, yl = total(1)
        y_ref[top, :] = yt
        y_ref[low, :] = yl
        part3[2] = (tdot(llm[...], y_ref[...]) + back[...]).astype(BF)
        send_sum(2)
        out_copy(1, y_ref, y_out).start()

    def y_parent():
        ypfull[mine, :] = (-(take_sum(1) + terms[...])).astype(BF)
        spread(1, ypfull)

    def diag_lower():
        dlfull[mine, :] = (dl_ref[mine, :] - take_sum(2)).astype(BF)
        spread(2, dlfull)

    def gather_upper():
        all_spread(0, dufull).wait_recv()
        out_copy(2, dufull, diagu_out).start()

    def gather_parent():
        all_spread(1, ypfull).wait_recv()
        out_copy(3, ypfull, yp_out).start()

    def gather_lower():
        all_spread(2, dlfull).wait_recv()
        out_copy(4, dlfull, diagl_out).start()

    def wait_ins():
        for i in ins[2:]:
            i.wait()

    def products(p, l):
        for o in range(1, CX):
            product(p, o, l)

    pl.when(jnp.logical_not(primary))(start_hops)
    late_home = is_kind["HO"]
    step("ev0", lambda: events(0.1, 0.2, 0.1, 0.1))
    step("mask", mask_own)
    step("ev1", lambda: events(11.9, 19.5, 10.9, 14.9))
    wait_ins()
    step("prod_u1", lambda: product(0, 0, 0))
    step("ev2", lambda: events(19.5, 23.9, 15.1, 19.0))
    step("prod_u4", lambda: products(0, 0))
    step("ev3", lambda: events(19.5, 28.0, 23.5, 27.4))
    step("prod_u2", lambda: product(0, 0, 1))
    step("ev4", lambda: events(19.5, 32.1, 27.7, 31.6))
    step("prod_u3", lambda: products(0, 1))
    step("ev5", lambda: events(99, 40.4, 36.2, 40.1))
    step("second", lambda: second(0))
    step("lprod_u3", lambda: products(1, 1), jnp.logical_not(late_home))
    step("ev6", lambda: events(99, 44.5, 44.6, 44.4))
    step("lprod_u3o", lambda: products(1, 1), late_home)
    step("x_final", x_final)
    step("ev7", lambda: events(99, 48.7, 44.6, 48.5))
    step("lprod_u4", lambda: products(1, 0))
    step("ev8", lambda: events(99, 53.0, 48.9, 52.8))
    step("lprod_u2", lambda: product(1, 0, 1))
    step("second_l", lambda: second(1))
    step("choose_send", choose_send)
    step("diag_upper", diag_upper)
    step("ev9", lambda: events(99, 99, 99, 99))
    step("lprod_u1", lambda: product(1, 0, 0))
    step("choose_take", choose_take)
    step("crossed", crossed)
    step("coupling", coupling)
    step("parent_terms", parent_terms)
    step("y_final", y_final)
    step("y_parent", y_parent)
    step("diag_lower", diag_lower)
    step("gather_upper", gather_upper)
    step("gather_parent", gather_parent)
    step("gather_lower", gather_lower)

    def finish():
        @pl.when(primary)
        def _():
            wait_sends()

        @pl.when(jnp.logical_not(primary))
        def _():
            for p in range(2):
                copy(ybuf.at[p], ybuf.at[p], h_ss.at[p], h_ss.at[p], rdev(r)).wait_send()

        def sent(sem, at):
            copy(at, at, sem, sem, rdev(r)).wait_send()

        for p in range(2):
            sent(ny_ss.at[p], near_y.at[p])
            sent(nx_ss.at[p], near_x.at[p, pl.ds(0, (CX - 1) * G)])
            sent(ly_ss.at[p], last_y.at[p, pl.ds(0, CX - 1)])
            sent(lx_ss.at[p], last_x.at[p])
        sent(xr_ss.at[0], xrow.at[pl.ds(0, CX - 1)])
        sent(ch_ss.at[0], chy)
        for k in range(3):
            all_red(k).wait_send()
        for i, buf in enumerate((dufull, ypfull, dlfull)):
            all_spread(i, buf).wait_send()
        all_dp().wait_send()
        for i, (src, dst) in enumerate(
            ((x_ref, x_out), (y_ref, y_out), (dufull, diagu_out), (ypfull, yp_out), (dlfull, diagl_out))
        ):
            out_copy(i, src, dst).wait()

    step("finish", finish)


def hand_out(*refs):
    k = (len(refs) - 2) // 3
    ins, outs, held = refs[:k], refs[k : 2 * k], refs[2 * k : 3 * k]
    in_s, out_s = refs[3 * k :]
    for i in range(k):
        pltpu.make_async_copy(ins[i], held[i], in_s.at[i]).start()
    for i in range(k):
        pltpu.make_async_copy(ins[i], held[i], in_s.at[i]).wait()
        pltpu.make_async_copy(held[i], outs[i], out_s.at[i]).start()
    for i in range(k):
        pltpu.make_async_copy(held[i], outs[i], out_s.at[i]).wait()


def on_device(G, R, C, a, lu, mu, du, ll, ml, par, lp, dl):
    h = lu.shape[0]
    n = G * R
    q = n // C
    S = B // n
    CX = C // G
    W = h // B
    H2 = h // 2
    hbm = pl.BlockSpec(memory_space=pl.ANY)
    sm = pl.BlockSpec(memory_space=pltpu.SMEM)
    dma = pltpu.SemaphoreType.DMA
    small = jax.ShapeDtypeStruct((B, B), BF)
    tall = jax.ShapeDtypeStruct((h, B), BF)
    vm = pltpu.VMEM
    made = pl.pallas_call(
        functools.partial(kernel, G, R, C),
        out_shape=(tall, small, tall, small, small),
        in_specs=[hbm, hbm, sm, hbm, hbm, sm, sm, hbm, hbm],
        out_specs=(hbm,) * 5,
        scratch_shapes=[
            vm(a.shape, BF), vm((h, B), BF), vm((h, B), BF), vm((B, B), F32), vm((B, B), F32), vm((B, B), BF),
            vm((h, B), BF), vm((h, B), BF),
            vm((2, h, B), BF),
            vm((2, R, h, B), BF),
            vm((2, q * C, h, B), BF),
            vm((2, C, h, B), F32),
            vm((2, C, h, B), BF),
            vm((2, CX, H2, B), BF),
            vm((2, CX * G, H2, B), BF),
            vm((2, CX, H2, B), BF),
            vm((2, H2, B), BF),
            vm((2, CX, H2, B), BF),
            vm((2, H2, B), BF),
            vm((q * h, B), BF),
            vm((h, B), BF), vm((h, B), BF),
            vm((CX, h, B), BF), vm((h, B), BF), vm((h, B), BF), vm((h, B), BF),
            vm((3, B, B), BF),
            vm((3, n, S, B), BF),
            vm((B, B), BF),
            vm((C, S, B), BF),
            vm((B, B), BF),
            vm((B, B), F32),
            vm((B, B), BF),
            vm((h, B), BF), vm((S, B), F32),
            dma((6,)), dma((5,)),
            dma((2,)), dma((2, W)), dma((2, 2)), dma((2, R, W)),
            dma((2, q * C, W)), dma((2, 2)), dma((2,)), dma((2, 1)),
            dma((2,)), dma((2, CX)), dma((2,)), dma((2, CX * G)),
            dma((2,)), dma((2, CX)), dma((2,)), dma((2,)),
            dma((1,)), dma((CX, W)), dma((1,)), dma((W,)),
            dma((3,)), dma((3,)), dma((4,)), dma((4,)),
        ],
        compiler_params=pltpu.CompilerParams(
            collective_id=0, has_side_effects=True, vmem_limit_bytes=60 * 1024 * 1024
        ),
    )(a, lu, mu, du, ll, ml, par, lp, dl)
    k = len(made)
    return pl.pallas_call(
        hand_out,
        out_shape=tuple(jax.ShapeDtypeStruct(v.shape, v.dtype) for v in made),
        in_specs=[hbm] * k,
        out_specs=(hbm,) * k,
        scratch_shapes=[vm(v.shape, v.dtype) for v in made] + [dma((k,)), dma((k,))],
    )(*made)


def solution(mesh):
    tall, wide = P(("grp", "row"), "col"), P(None, "col")
    return jax.shard_map(
        functools.partial(
            on_device, mesh.shape["grp"], mesh.shape["row"], mesh.shape["col"]
        ),
        mesh=mesh,
        in_specs=(tall, tall, P(), wide, tall, P(), P(), wide, wide),
        out_specs=(tall, wide, tall, wide, wide),
        check_vma=False,
    )
```

```python
import functools

import jax
import jax.numpy as jnp
from jax import lax
from jax.experimental import pallas as pl
from jax.experimental.pallas import tpu as pltpu
from jax.sharding import PartitionSpec as P

B = 256
MESH = pl.DeviceIdType.MESH
BF = jnp.bfloat16
F32 = jnp.float32


def tdot(a, b):
    return lax.dot_general(a, b, (((0,), (0,)), ((), ())), preferred_element_type=F32)


def land(*conds):
    out = conds[0]
    for k in conds[1:]:
        out = jnp.logical_and(out, k)
    return out


TAU = 1.4
HI, HO, AI, AO = range(4)
OWN, AWAY_OWN, TRANSIT, ARRIVE = range(4)
HOME, AWAY = range(2)
FAR, NEAR = range(2)
ALONG, CROSS, THROUGH = range(3)


def plan(kind, R, q, CX, W):
    ev = []

    def add(t, name, *args, slope=TAU):
        for w in range(W):
            ev.append((t + slope * w, name, args, w))

    def at(t, name, *args):
        add(t, name, *args, slope=0.001)

    others = range(1, CX)
    inner = kind in (HI, AI)
    at_home = kind in (HI, HO)
    if CX != 2:
        for p, l in ((0, 0), (0, 1), (1, 0), (1, 1)):
            if at_home:
                for part in (FAR, NEAR):
                    at(0, OWN, p, l, part)
            else:
                at(0, AWAY_OWN, p, l)
        for p in range(2):
            for s in range(1, R):
                for side in range(2):
                    at(1 + p + s / R, TRANSIT, p, s, side)
            t = (5, 33)[p]
            if at_home:
                for part in (FAR, NEAR):
                    for o in others:
                        for l in range(2):
                            at(t, ARRIVE, p, HOME, 0, o, l, part)
            for l in range(2):
                for o in range(CX):
                    for i in range(1 if at_home else 0, q):
                        at(t + 1 + l + 0.1 * o, ARRIVE, p, AWAY if not at_home else HOME, i, o, l, FAR)
        return sorted(ev, key=lambda e: e[0])
    if at_home:
        at(0, OWN, 0, 0, FAR)
        for s in range(1, R):
            for side in range(2):
                add((0 if inner else 0.1) + 3.9 * s, TRANSIT, 0, s, side)
                add(9.1 + 4 * s if inner else 16.5 + 4.2 * s, TRANSIT, 1, s, side)
        if inner:
            add(4.03, OWN, 0, 1, FAR)
            at(20.4, OWN, 0, 0, NEAR)
            at(20.3, OWN, 0, 1, NEAR)
            at(24.8, OWN, 1, 1, FAR)
            at(28.7, OWN, 1, 0, FAR)
            at(28.8, OWN, 1, 1, NEAR)
            at(28.9, OWN, 1, 0, NEAR)
        else:
            at(0.1, OWN, 0, 0, NEAR)
            add(4.0, OWN, 0, 1, FAR)
            add(4.01, OWN, 0, 1, NEAR)
            at(18.2, OWN, 1, 1, FAR)
            at(18.3, OWN, 1, 1, NEAR)
            at(18.4, OWN, 1, 0, FAR)
            at(18.5, OWN, 1, 0, NEAR)
        for o in others:
            add(4.05, ARRIVE, 0, HOME, 0, o, 0, FAR)
            add(8.0, ARRIVE, 0, HOME, 0, o, 1, FAR)
            if inner:
                at(12.4, ARRIVE, 0, HOME, 0, o, 0, NEAR)
                at(12.8, ARRIVE, 0, HOME, 0, o, 1, NEAR)
                at(17, ARRIVE, 1, HOME, 0, o, 1, FAR)
                at(19.9, ARRIVE, 1, HOME, 0, o, 0, FAR)
                at(20.35, ARRIVE, 1, HOME, 0, o, 1, NEAR)
                at(25.1, ARRIVE, 1, HOME, 0, o, 0, NEAR)
            else:
                add(8.01, ARRIVE, 0, HOME, 0, o, 1, NEAR)
                at(11.5, ARRIVE, 0, HOME, 0, o, 0, NEAR)
                add(15.2, ARRIVE, 1, HOME, 0, o, 1, FAR)
                add(15.21, ARRIVE, 1, HOME, 0, o, 1, NEAR)
                at(20.2, ARRIVE, 1, HOME, 0, o, 0, FAR)
                at(20.3, ARRIVE, 1, HOME, 0, o, 0, NEAR)
        for i in range(1, q):
            first = (15.4, 10.9, 12.5, 16.5) if inner else (41.6, 33.2, 20.5, 16.2)
            last = (29.2, 25.0, 20.7, 33.5) if inner else (54.3, 50.1, 37.4, 45.8)
            for p, (t1, t2, t3, t4) in ((0, first), (1, last)):
                flat = 0.001 if inner and p == 0 else TAU
                add(t1, ARRIVE, p, HOME, i, 0, 0, FAR, slope=flat)
                add(t2, ARRIVE, p, HOME, i, 0, 1, FAR, slope=flat)
                for o in others:
                    add(t3, ARRIVE, p, HOME, i, o, 1, FAR)
                    add(t4, ARRIVE, p, HOME, i, o, 0, FAR)
    else:
        at(0, AWAY_OWN, 0, 0)
        for s in range(1, R):
            for side in range(2):
                add(0.1 + 3.9 * s, TRANSIT, 0, s, side)
                add(11.5 + 3.9 * s, TRANSIT, 1, s, side)
        add(4.1, AWAY_OWN, 0, 1)
        add(8.5, AWAY_OWN, 1, 1)
        at(11.6, AWAY_OWN, 1, 0)
        d = 0 if inner else 3.9
        for i in range(q):
            add(4.05 + d + 20.75 * i, ARRIVE, 0, AWAY, i, 0, 0, FAR)
            add(8.0 + d + 8.4 * i, ARRIVE, 0, AWAY, i, 0, 1, FAR)
            add(37.5 + d + 4.2 * i, ARRIVE, 1, AWAY, i, 0, 1, FAR)
            add(46 + d + 4.2 * i, ARRIVE, 1, AWAY, i, 0, 0, FAR)
            for o in others:
                add(8.2 + d + 4 * i, ARRIVE, 0, AWAY, i, o, 0, FAR)
                add(12.1 + d + 8.5 * i, ARRIVE, 0, AWAY, i, o, 1, FAR)
                at((36.1 if inner else 36.3) + 0.01 * i, ARRIVE, 1, AWAY, i, o, 0, FAR)
                add(29 + d + 4.2 * i, ARRIVE, 1, AWAY, i, o, 1, FAR)
    return sorted(ev, key=lambda e: e[0])


def kernel(
    G, R, C,
    a_in, lu_in, mu_in, du_in, ll_in, ml_in, par_in, lp_in, dl_in,
    x_out, diagu_out, y_out, yp_out, diagl_out,
    a_ref, lu_ref, ll_ref, du_ref, dl_ref, lp_ref, mu_ref, ml_ref, par_ref,
    x_ref, y_ref, ybuf, zbuf, col, acc, part, near_y, near_x, sent_y, sent_x, last_y, last_x,
    rhs, lum, llm, xrow, yrow, sel_y, ch_y, sel_x, ch_x, chosen, part3, red, dufull, dpar, ypfull, back, dlfull,
    linked, terms, in_s, out_s,
    h_ss, h_rs, t_ss, t_rs, c_rs, v_ss, r_ss, x_ss,
    ny_ss, ny_rs, nx_ss, nx_rs, ly_ss, ly_rs, lx_ss, lx_rs,
    k_ss, xr_rs, yr_rs, cy_rs, cx_rs,
    red_ss, red_rs, s_ss, s_rs,
):
    g, z, c = lax.axis_index("grp"), lax.axis_index("row"), lax.axis_index("col")
    n = G * R
    q = n // C
    CX = C // G
    y, x = lax.div(c, CX), lax.rem(c, CX)
    r = g * R + z
    h = lu_ref.shape[0]
    hb = W = h // B
    S = B // n
    H2 = h // 2
    panels = (lu_ref, ll_ref)
    masks = (mu_ref, ml_ref)
    primary = y == g
    zh = lax.div(z, q)
    home = zh == x
    oy = 1 - y

    def rdev(i):
        return (lax.div(i, R), lax.rem(i, R), c)

    def pdev(yy, xx):
        return (g, z, yy * CX + xx)

    def xo(o):
        return lax.rem(x + o, CX)

    def copy(src, dst, ss, rs, dev):
        return pltpu.make_async_remote_copy(
            src_ref=src, dst_ref=dst, send_sem=ss, recv_sem=rs, device_id=dev, device_id_type=MESH
        )

    ins = [
        pltpu.make_async_copy(src, dst, in_s.at[i])
        for i, (src, dst) in enumerate(
            (
                (lu_in, lu_ref), (ll_in, ll_ref), (mu_in, mu_ref), (ml_in, ml_ref), (par_in, par_ref),
                (a_in, a_ref), (lp_in, lp_ref), (du_in, du_ref), (dl_in, dl_ref),
            )
        )
    ]
    barrier = pltpu.get_barrier_semaphore()
    for o in range(1, n):
        pl.semaphore_signal(barrier, inc=1, device_id=rdev(lax.rem(r + o, n)), device_id_type=MESH)
    for o in range(1, C):
        pl.semaphore_signal(
            barrier, inc=1, device_id=(g, z, lax.rem(c + o, C)), device_id_type=MESH
        )
    for i in ins:
        i.start()
    for i in ins[:2]:
        i.wait()
    pl.semaphore_wait(barrier, n - 1 + C - 1)

    log = []

    def cut(w):
        return pl.ds(w * B, B)

    edge = (z < R - 1, z > 0)
    away = jnp.logical_not(home)
    outer = jnp.logical_or(z == 0, z == R - 1)
    far = ((zh + 1) * q < R, zh > 0)
    zj = lax.rem(z, q)

    def side_dev(side):
        return (g, z + 1 if side == 0 else z - 1, c)

    def col_u(o, l):
        return (y if l == 0 else oy) * CX + xo(o)

    def hop_copy(p, w):
        return copy(
            panels[p].at[cut(w), :], ybuf.at[p, cut(w), :], h_ss.at[p], h_rs.at[p, w],
            (g, z, g * CX + x),
        )

    def own_src(p, l, w):
        return panels[p].at[cut(w), :] if l == 0 else ybuf.at[p, cut(w), :]

    def at_col(p, j, u, w):
        return col.at[p, j * C + u, cut(w), :]

    def along(p, j, u, side, w, src):
        return (ALONG, p, side), lambda: copy(
            src, at_col(p, j, u, w), v_ss.at[p, side], c_rs.at[p, j * C + u, w], side_dev(side)
        )

    def relay(p, j, u, w, src):
        return None, lambda: copy(
            src, at_col(p, j, u, w), r_ss.at[p], c_rs.at[p, j * C + u, w], (1 - g, z, c)
        )

    def cross(p, z0, l, w, src):
        u, j = col_u(0, l), lax.rem(z0, q)
        return (CROSS, p, 0), lambda: copy(
            src, at_col(p, j, u, w), x_ss.at[p, 0], c_rs.at[p, j * C + u, w],
            pdev(y, lax.div(z0, q)),
        )

    def through(p, z0, side, w, src):
        return (THROUGH, p, side), lambda: copy(
            src, zbuf.at[p, z0, cut(w), :], t_ss.at[p, side], t_rs.at[p, z0, w], side_dev(side)
        )

    near_side = (lax.div(z + 1, q) == x, lax.div(z - 1 + q, q) == x + 1)

    def own(p, l, part, w):
        u, src = col_u(0, l), own_src(p, l, w)

        def sides(near):
            return [
                (
                    land(edge[k], near_side[k] if near else jnp.logical_not(near_side[k])),
                    along(p, zj, u, k, w, src),
                )
                for k in range(2)
            ]

        if part == NEAR:
            return home, None, sides(True), None

        def local():
            k = pltpu.make_async_copy(src, at_col(p, zj, u, w), c_rs.at[p, zj * C + u, w])
            k.start()
            k.wait()

        outs = sides(False) + [(None, relay(p, zj, u, w, src))]
        return home, (lambda: hop_copy(p, w)) if l == 1 else None, outs, local

    def away_own(p, l, w):
        src = own_src(p, l, w)
        outs = [(None, cross(p, z, l, w, src))]
        if l == 0:
            outs += [(far[side], through(p, z, side, w, src)) for side in range(2)]
        return away, (lambda: hop_copy(p, w)) if l == 1 else None, outs, None

    def transit(p, s, side, w):
        z0 = z - s if side == 0 else z + s
        b0 = lax.div(z0, q)
        ok = z0 >= 0 if side == 0 else z0 < R
        path = (b0 + 1) * q < R if side == 0 else b0 > 0
        at = zbuf.at[p, z0, cut(w), :]
        outs = [(edge[side], through(p, z0, side, w, at)), (zh != b0, cross(p, z0, 0, w, at))]
        return land(ok, path, b0 != x), through(p, z0, side, w, at)[1], outs, None

    def arrive(p, kind, i, o, l, part, w):
        j = lax.rem(zj + i, q) if kind == HOME else jnp.where(z < x * q, i, q - 1 - i)
        z0 = x * q + j
        u = col_u(o, l)
        at = at_col(p, j, u, w)
        side = (land(z0 <= z, edge[0]), land(z0 >= z, edge[1]))
        late = o != 0 and l == 0
        outs = []
        for k in range(2):
            step_to = along(p, j, u, k, w, at)
            if kind == AWAY:
                if not late:
                    outs.append((side[k], step_to))
            elif i == 0:
                if part == NEAR:
                    outs.append((land(side[k], near_side[k]), step_to))
                elif not late:
                    outs.append((land(side[k], jnp.logical_not(near_side[k])), step_to))
            else:
                outs.append((land(side[k], near_side[k]) if late else side[k], step_to))
        live = home if kind == HOME else away
        if part == NEAR:
            return live, None, outs, None
        outs.append((None, relay(p, j, u, w, at)))
        return live, relay(p, j, u, w, at)[1], outs, None

    def emit(f, *args):
        log.append((f, args))
        live, first, outs, local = f(*args)

        def body():
            if first is not None:
                first().wait_recv()
            for cond, (_, make) in outs:
                if cond is None:
                    make().start()
                else:
                    pl.when(cond)(lambda: make().start())
            if local is not None:
                local()

        pl.when(live)(body)

    def wait_blocks(sem, p, k):
        at = col.at[p, pl.ds(0, k)]
        copy(at, at, sem, sem, rdev(r)).wait_send()

    def wait_sends():
        for p in range(2):
            wait_blocks(r_ss.at[p], p, q * C)
        count = {}
        for f, args in dict.fromkeys(log):
            if args[-1] == 0:
                live, _, outs, _ = f(*args)
                for cond, (key, _) in outs:
                    if key is not None:
                        on = live if cond is None else land(live, cond)
                        count[key] = count.get(key, 0) + jnp.where(on, 1, 0)
        for (kind, p, side), number in sorted(count.items()):
            sem = (v_ss, x_ss, t_ss)[kind].at[p, side]
            for k in range(1, (q * C, R + G, R)[kind] + 1):
                pl.when(number == k)(lambda: wait_blocks(sem, p, k))

    handlers = (own, away_own, transit, arrive)
    kinds = (HI, HO, AI, AO)
    timed = [plan(k, R, q, CX, W) for k in kinds]
    is_kind = (
        land(home, jnp.logical_not(outer)), land(home, outer),
        land(away, jnp.logical_not(outer)), land(away, outer),
    )

    def events(*until):
        for k, to in zip(kinds, until):
            now = [e for e in timed[k] if e[0] < to]
            timed[k] = timed[k][len(now):]
            if now:
                @pl.when(land(primary, is_kind[k]))
                def _():
                    for _, name, args, w in now:
                        emit(handlers[name], *args, w)

    def kd(o, l):
        return l * CX + o

    def ny_copy(p, o):
        return copy(
            part.at[p, kd(o, 1), pl.ds(0, H2), :], near_y.at[p, o], ny_ss.at[p], ny_rs.at[p, o],
            pdev(oy, x),
        )

    def nx_copy(p, o, l):
        i = (CX - o) * G + l
        return copy(
            part.at[p, kd(o, l), pl.ds(H2, H2), :], near_x.at[p, i], nx_ss.at[p], nx_rs.at[p, i],
            pdev(y, xo(o)),
        )

    def ly_copy(p, o):
        return copy(
            sent_y.at[p, o], last_y.at[p, CX - o], ly_ss.at[p], ly_rs.at[p, CX - o],
            pdev(y, xo(o)),
        )

    def lx_copy(p):
        return copy(sent_x.at[p], last_x.at[p], lx_ss.at[p], lx_rs.at[p], pdev(oy, x))

    def product(p, o, l):
        u = (y if l == 0 else oy) * CX + xo(o)
        k = kd(o, l)

        @pl.when(jnp.logical_not(primary))
        def _():
            for j in range(q):
                for w in range(W):
                    relay(p, j, u, w, at_col(p, j, u, w))[1]().wait_recv()

        @pl.loop(0, q * hb)
        def _(i):
            j, t = lax.div(i, hb), lax.rem(i, hb)
            keep = masks[p][u, c * q * hb + i] > 0
            rows = pl.ds(pl.multiple_of(t * B, B), B)
            blk = col[p, j * C + u, rows, :]
            rhs[pl.ds(pl.multiple_of(i * B, B), B), :] = jnp.where(keep, blk, jnp.zeros_like(blk))

        @pl.loop(0, 2)
        def _(t):
            rows = pl.ds(pl.multiple_of(t * H2, H2), H2)
            v = jnp.dot(a_ref[rows, :], rhs[...], preferred_element_type=F32)
            acc[p, k, rows, :] = v
            part[p, k, rows, :] = v.astype(BF)

        if l == 1:
            ny_copy(p, o).start()
        if o != 0:
            nx_copy(p, o, l).start()

    top, low = pl.ds(0, H2), pl.ds(H2, H2)

    def second(p):
        for o in range(1, CX):
            ny_copy(p, o).wait_recv()
            sent_y[p, o] = (acc[p, kd(o, 0), top, :] + near_y[p, o].astype(F32)).astype(BF)
            ly_copy(p, o).start()
        v = acc[p, kd(0, 1), low, :]
        for o in range(1, CX):
            nx_copy(p, CX - o, 1).wait_recv()
            v = v + near_x[p, o * G + 1].astype(F32)
        sent_x[p] = v.astype(BF)
        lx_copy(p).start()

    def total(p):
        ny_copy(p, 0).wait_recv()
        v = acc[p, 0, top, :] + near_y[p, 0].astype(F32)
        for o in range(1, CX):
            ly_copy(p, CX - o).wait_recv()
            v = v + last_y[p, o].astype(F32)
        w = acc[p, 0, low, :]
        for o in range(1, CX):
            nx_copy(p, CX - o, 0).wait_recv()
            w = w + near_x[p, o * G].astype(F32)
        lx_copy(p).wait_recv()
        w = w + last_x[p].astype(F32)
        return (-v).astype(BF), (-w).astype(BF)

    def red_copy(k, o):
        i = lax.rem(r + o, n)
        return copy(
            part3.at[k, pl.ds(pl.multiple_of(i * S, S), S), :], red.at[k, r],
            red_ss.at[k], red_rs.at[k], rdev(i),
        )

    def send_sum(k):
        red[k, r] = part3[k, pl.ds(pl.multiple_of(r * S, S), S), :]
        for o in range(1, n):
            red_copy(k, o).start()

    def all_red(k):
        at = red.at[k, pl.ds(0, n - 1)]
        return copy(at, at, red_ss.at[k], red_rs.at[k], rdev(r))

    def take_sum(k):
        all_red(k).wait_recv()
        v = red[k, 0].astype(F32)
        for i in range(1, n):
            v = v + red[k, i].astype(F32)
        return v

    mine = pl.ds(pl.multiple_of(r * S, S), S)

    def spread(i, buf):
        for o in range(1, n):
            copy(
                buf.at[mine, :], buf.at[mine, :], s_ss.at[i], s_rs.at[i], rdev(lax.rem(r + o, n))
            ).start()

    def all_spread(i, buf):
        at = buf.at[pl.ds(0, (n - 1) * S), :]
        return copy(at, at, s_ss.at[i], s_rs.at[i], rdev(r))

    def dp_copy(o):
        return copy(
            dpar.at[c], dpar.at[c], s_ss.at[3], s_rs.at[3], (g, z, lax.rem(c + o, C))
        )

    def all_dp():
        at = dpar.at[pl.ds(0, C - 1)]
        return copy(at, at, s_ss.at[3], s_rs.at[3], rdev(r))

    TR = H2 // 2

    def tile(t):
        return pl.ds(t * TR, TR)

    def low_tile(t):
        return pl.ds(H2 + t * TR, TR)

    def xr_copy(o, t):
        return copy(
            x_ref.at[tile(t), :], xrow.at[CX - o, tile(t), :], k_ss.at[0], xr_rs.at[CX - o, t],
            pdev(y, xo(o)),
        )

    def yr_copy(t):
        return copy(x_ref.at[low_tile(t), :], yrow.at[tile(t), :], k_ss.at[1], yr_rs.at[t], pdev(oy, x))

    def cy_copy(t):
        return copy(sel_y.at[tile(t), :], ch_y.at[tile(t), :], k_ss.at[2], cy_rs.at[t], pdev(oy, x))

    def cx_copy(o, t):
        return copy(
            sel_x.at[o, tile(t), :], ch_x.at[CX - o, tile(t), :], k_ss.at[3], cx_rs.at[CX - o, t],
            pdev(y, xo(o)),
        )

    def pick_row(who, v, t):
        for o in range(CX):
            block = x_ref[tile(t), :] if o == 0 else xrow[o, tile(t), :]
            v = jnp.where(who == y * CX + xo(o), block, v)
        return v

    def pick_pair(who, v, t):
        v = jnp.where(who == oy * CX + x, yrow[tile(t), :], v)
        return jnp.where(who == c, x_ref[low_tile(t), :], v)

    def out_copy(i, src, dst):
        return pltpu.make_async_copy(src, dst, out_s.at[i])

    def step(f, cond=None):
        if cond is None:
            f()
        else:
            pl.when(cond)(f)

    def start_hops():
        for p in range(2):
            for w in range(W):
                hop_copy(p, w).start()

    def mask_own():
        for i in ins[2:5]:
            i.wait()

        @pl.loop(0, hb)
        def _(t):
            rows = pl.ds(pl.multiple_of(t * B, B), B)
            ub, lb = lu_ref[rows, :], ll_ref[rows, :]
            lum[rows, :] = jnp.where(mu_ref[c, r * hb + t] > 0, ub, jnp.zeros_like(ub))
            llm[rows, :] = jnp.where(ml_ref[c, r * hb + t] > 0, lb, jnp.zeros_like(lb))

    def x_final():
        xt, xl = total(0)
        x_ref[top, :] = xt
        x_ref[low, :] = xl
        for t in range(2):
            for o in range(1, CX):
                xr_copy(o, t).start()
            yr_copy(t).start()
        out_copy(0, x_ref, x_out).start()
        part3[0] = tdot(lum[...], x_ref[...]).astype(BF)
        send_sum(0)

    def choose_send():
        for t in range(2):
            for o in range(1, CX):
                xr_copy(CX - o, t).wait_recv()
            sel_y[tile(t), :] = pick_row(par_ref[oy * CX + x], x_ref[tile(t), :], t)
            cy_copy(t).start()
            yr_copy(t).wait_recv()
            for o in range(1, CX):
                sel_x[o, tile(t), :] = pick_pair(par_ref[y * CX + xo(o)], x_ref[low_tile(t), :], t)
                cx_copy(o, t).start()

    def diag_upper():
        dslice = (du_ref[mine, :] - take_sum(0)).astype(BF)
        dufull[mine, :] = dslice
        dpar[c] = dslice
        for o in range(1, C):
            dp_copy(o).start()
        spread(0, dufull)

    def choose_take():
        here = par_ref[c]
        for t in range(2):
            cy_copy(t).wait_recv()
            chosen[tile(t), :] = pick_row(here, ch_y[tile(t), :], t)
            v = x_ref[low_tile(t), :]
            for o in range(1, CX):
                cx_copy(CX - o, t).wait_recv()
                v = jnp.where(lax.rem(here, CX) == xo(o), ch_x[o, tile(t), :], v)
            chosen[low_tile(t), :] = pick_pair(here, v, t)

    def crossed():
        part3[1] = tdot(chosen[...], llm[...]).astype(BF)
        send_sum(1)

    def coupling():
        @pl.loop(0, hb)
        def _(t):
            rows = pl.ds(pl.multiple_of(t * B, B), B)
            v = jnp.dot(chosen[rows, :], lp_ref[...], preferred_element_type=F32)
            acc[1, 0, rows, :] += v
            linked[rows, :] = v.astype(BF)

        back[...] = tdot(linked[...], llm[...])

    def parent_terms():
        all_dp().wait_recv()
        v = jnp.dot(dpar[par_ref[c]], lp_ref[...], preferred_element_type=F32)
        terms[...] = v
        part3[3] = tdot(lp_ref[mine, :], v.astype(BF)).astype(BF)
        send_sum(3)

    def y_final():
        yt, yl = total(1)
        y_ref[top, :] = yt
        y_ref[low, :] = yl
        part3[2] = (tdot(llm[...], y_ref[...]) - back[...]).astype(BF)
        send_sum(2)
        out_copy(1, y_ref, y_out).start()

    def y_parent():
        ypfull[mine, :] = (-(take_sum(1) + terms[...])).astype(BF)
        spread(1, ypfull)

    def diag_lower():
        dlfull[mine, :] = (dl_ref[mine, :] - take_sum(2) + take_sum(3)).astype(BF)
        spread(2, dlfull)

    def gather_upper():
        all_spread(0, dufull).wait_recv()
        out_copy(2, dufull, diagu_out).start()

    def gather_parent():
        all_spread(1, ypfull).wait_recv()
        out_copy(3, ypfull, yp_out).start()

    def gather_lower():
        all_spread(2, dlfull).wait_recv()
        out_copy(4, dlfull, diagl_out).start()

    def wait_ins():
        for i in ins[5:]:
            i.wait()

    def products(p, l):
        for o in range(1, CX):
            product(p, o, l)

    pl.when(jnp.logical_not(primary))(start_hops)
    ho, hi = is_kind[HO], is_kind[HI]
    no = jnp.logical_not(ho)
    step(lambda: events(0.1, 0.2, 0.1, 0.1))
    step(mask_own)
    step(lambda: events(15.5, 19.1, 15.1, 19.0))
    wait_ins()
    step(lambda: products(0, 1), hi)
    step(lambda: product(0, 0, 1), hi)
    step(lambda: product(0, 0, 0), hi)
    step(lambda: events(20.5, 19.1, 15.1, 19.0))
    step(lambda: products(0, 0))
    step(lambda: events(20.5, 23.4, 19.3, 23.2))
    step(lambda: product(0, 0, 1), away)
    step(lambda: products(0, 1), ho)
    step(lambda: events(20.5, 30.0, 23.5, 27.4))
    step(lambda: products(0, 1), away)
    step(lambda: events(20.5, 36.1, 27.7, 31.6))
    step(lambda: product(0, 0, 0), away)
    step(lambda: product(0, 0, 1), ho)
    step(lambda: events(25.3, 36.1, 33.0, 31.6))
    step(lambda: second(0))
    step(lambda: events(99, 40.3, 36.2, 36.4))
    step(lambda: products(1, 0), no)
    step(lambda: events(99, 40.3, 36.2, 40.1))
    step(lambda: products(1, 1))
    step(lambda: events(99, 44.5, 44.6, 44.4))
    step(lambda: product(0, 0, 0), ho)
    step(x_final)
    step(lambda: events(99, 48.7, 44.6, 48.5))
    step(lambda: product(1, 0, 1), no)
    step(lambda: second(1), no)
    step(lambda: products(1, 0), ho)
    step(choose_send, ho)
    step(lambda: events(99, 53.0, 48.9, 52.8))
    step(choose_send, no)
    step(diag_upper, is_kind[AO])
    step(lambda: product(1, 0, 1), ho)
    step(lambda: second(1), ho)
    step(lambda: events(99, 99, 99, 99))
    step(diag_upper, jnp.logical_not(is_kind[AO]))
    step(lambda: product(1, 0, 0))
    step(choose_take)
    step(crossed)
    step(coupling)
    step(y_final)
    step(parent_terms)
    step(y_parent)
    step(diag_lower)
    step(gather_upper)
    step(gather_parent)
    step(gather_lower)

    def finish():
        @pl.when(primary)
        def _():
            wait_sends()

        @pl.when(jnp.logical_not(primary))
        def _():
            for p in range(2):
                copy(ybuf.at[p], ybuf.at[p], h_ss.at[p], h_ss.at[p], rdev(r)).wait_send()

        def sent(sem, at):
            copy(at, at, sem, sem, rdev(r)).wait_send()

        for p in range(2):
            sent(ny_ss.at[p], near_y.at[p])
            sent(nx_ss.at[p], near_x.at[p, pl.ds(0, (CX - 1) * G)])
            sent(ly_ss.at[p], last_y.at[p, pl.ds(0, CX - 1)])
            sent(lx_ss.at[p], last_x.at[p])
        sent(k_ss.at[0], xrow.at[pl.ds(0, CX - 1)])
        sent(k_ss.at[1], yrow)
        sent(k_ss.at[2], ch_y)
        sent(k_ss.at[3], ch_x.at[pl.ds(0, CX - 1)])
        for k in range(4):
            all_red(k).wait_send()
        for i, buf in enumerate((dufull, ypfull, dlfull)):
            all_spread(i, buf).wait_send()
        all_dp().wait_send()
        for i, (src, dst) in enumerate(
            ((x_ref, x_out), (y_ref, y_out), (dufull, diagu_out), (ypfull, yp_out), (dlfull, diagl_out))
        ):
            out_copy(i, src, dst).wait()

    step(finish)


def hand_out(*refs):
    k = (len(refs) - 2) // 3
    ins, outs, held = refs[:k], refs[k : 2 * k], refs[2 * k : 3 * k]
    in_s, out_s = refs[3 * k :]
    for i in range(k):
        pltpu.make_async_copy(ins[i], held[i], in_s.at[i]).start()
    for i in range(k):
        pltpu.make_async_copy(ins[i], held[i], in_s.at[i]).wait()
        pltpu.make_async_copy(held[i], outs[i], out_s.at[i]).start()
    for i in range(k):
        pltpu.make_async_copy(held[i], outs[i], out_s.at[i]).wait()


def on_device(G, R, C, a, lu, mu, du, ll, ml, par, lp, dl):
    h = lu.shape[0]
    n = G * R
    q = n // C
    S = B // n
    CX = C // G
    W = h // B
    H2 = h // 2
    hbm = pl.BlockSpec(memory_space=pl.ANY)
    dma = pltpu.SemaphoreType.DMA
    small = jax.ShapeDtypeStruct((B, B), BF)
    tall = jax.ShapeDtypeStruct((h, B), BF)
    vm = pltpu.VMEM
    made = pl.pallas_call(
        functools.partial(kernel, G, R, C),
        out_shape=(tall, small, tall, small, small),
        in_specs=[hbm] * 9,
        out_specs=(hbm,) * 5,
        scratch_shapes=[
            vm(a.shape, BF), vm((h, B), BF), vm((h, B), BF), vm((B, B), F32), vm((B, B), F32), vm((B, B), BF),
            pltpu.SMEM(mu.shape, mu.dtype), pltpu.SMEM(ml.shape, ml.dtype), pltpu.SMEM(par.shape, par.dtype),
            vm((h, B), BF), vm((h, B), BF),
            vm((2, h, B), BF),
            vm((2, R, h, B), BF),
            vm((2, q * C, h, B), BF),
            vm((2, C, h, B), F32),
            vm((2, C, h, B), BF),
            vm((2, CX, H2, B), BF),
            vm((2, CX * G, H2, B), BF),
            vm((2, CX, H2, B), BF),
            vm((2, H2, B), BF),
            vm((2, CX, H2, B), BF),
            vm((2, H2, B), BF),
            vm((q * h, B), BF),
            vm((h, B), BF), vm((h, B), BF),
            vm((CX, H2, B), BF), vm((H2, B), BF), vm((H2, B), BF), vm((H2, B), BF),
            vm((CX, H2, B), BF), vm((CX, H2, B), BF), vm((h, B), BF),
            vm((4, B, B), BF),
            vm((4, n, S, B), BF),
            vm((B, B), BF),
            vm((C, S, B), BF),
            vm((B, B), BF),
            vm((B, B), F32),
            vm((B, B), BF),
            vm((h, B), BF), vm((S, B), F32),
            dma((9,)), dma((5,)),
            dma((2,)), dma((2, W)), dma((2, 2)), dma((2, R, W)),
            dma((2, q * C, W)), dma((2, 2)), dma((2,)), dma((2, 1)),
            dma((2,)), dma((2, CX)), dma((2,)), dma((2, CX * G)),
            dma((2,)), dma((2, CX)), dma((2,)), dma((2,)),
            dma((4,)), dma((CX, 2)), dma((2,)), dma((2,)), dma((CX, 2)),
            dma((4,)), dma((4,)), dma((4,)), dma((4,)),
        ],
        compiler_params=pltpu.CompilerParams(
            collective_id=0, has_side_effects=True, vmem_limit_bytes=60 * 1024 * 1024
        ),
    )(a, lu, mu, du, ll, ml, par, lp, dl)
    k = len(made)
    return pl.pallas_call(
        hand_out,
        out_shape=tuple(jax.ShapeDtypeStruct(v.shape, v.dtype) for v in made),
        in_specs=[hbm] * k,
        out_specs=(hbm,) * k,
        scratch_shapes=[vm(v.shape, v.dtype) for v in made] + [dma((k,)), dma((k,))],
    )(*made)


def solution(mesh):
    tall, wide = P(("grp", "row"), "col"), P(None, "col")
    return jax.shard_map(
        functools.partial(
            on_device, mesh.shape["grp"], mesh.shape["row"], mesh.shape["col"]
        ),
        mesh=mesh,
        in_specs=(tall, tall, P(), wide, tall, P(), P(), wide, wide),
        out_specs=(tall, wide, tall, wide, wide),
        check_vma=False,
    )
```
